32 devices in a mesh: row: 4 (over y, x), col: 8 (over z, core).
Axes of the slice: x: 2, y: 2, z: 4, core: 2. Of those that a mesh axis runs over, the one named last changes fastest.
Arguments:
- gains: float32 [512, 8, 256], P(('row', 'col')), may hold values from -6 to 6
- coherency: bfloat16 [512, 512, 8, 1, 256], P('row', 'col'), may hold values from -6 to 6
- cotangent: bfloat16 [512, 512, 8, 1, 8], P('row', 'col'), may hold values from -0.099609375 to 0.099609375
- flags: int32 [512, 512, 1], P('row', 'col'), may hold values 0 or 1
- station_slot: int32 [512], replicated, may hold values from 0 to 511, as said below
Outputs:
- gain_grad: float32 [512, 8, 256], P(('row', 'col'))
The draws below stay inside these ranges and needn't reach their ends.
Inputs may be any that keep to these rules, and one draw needn't show every extreme that they name: `station_slot`: each station appears in exactly one slot; in every aligned block of 16 consecutive slots the stations lie with 16 different holders, station s being held by the device of index s // 16 in the order of row+col.
All inputs are finite; a program needn't handle non-finite values. No bound on the sum of `flags` on one device may be relied on, other than what follows from the above.
Results may differ from the reference program's by a relative error of at most 0.0003.
Values sent between devices are 32-bit elements; how exact they have to be, the bound alone decides.
A program may use at most 128 MiB of HBM per device.

```python
import jax
import jax.numpy as jnp
from jax import lax

S = 512
GROUPS = 32
SD = 16
DIR = 32
CH = 8
TI = 1


def draw_station_slot(key, part):
    keys = jax.random.split(jax.random.fold_in(key, 17), 3)
    order = jax.random.permutation(keys[0], GROUPS).astype(jnp.int32)
    within = jax.random.randint(keys[1], (GROUPS,), 0, SD).astype(jnp.int32)
    offset = jax.random.randint(keys[2], (GROUPS,), 0, SD).astype(jnp.int32)
    stride = GROUPS // SD
    blocks = jnp.arange(GROUPS, dtype=jnp.int32)[:, None]
    places = jnp.arange(SD, dtype=jnp.int32)[None, :]
    holder = (order[blocks] + places * stride) % GROUPS
    number = (places + within[holder]) % SD
    station = holder * SD + number
    position = (places + offset[blocks]) % SD
    block_ids = jnp.broadcast_to(blocks, (GROUPS, SD))
    filled = jnp.zeros((GROUPS, SD), jnp.int32).at[block_ids, position].set(station)
    return filled.reshape(GROUPS * SD).astype(jnp.int32)


def plant(array, key, low, largest):
    shape = array.shape
    spot = [jax.random.randint(jax.random.fold_in(key, axis), (), 0, shape[axis]) for axis in range(len(shape))]
    array = array.at[tuple(spot)].set(low)
    longest = shape.index(max(shape))
    spot[longest] = (spot[longest] + 1) % shape[longest]
    return array.at[tuple(spot)].set(largest)


def level_of(stream_key, extent, cuts, low, top_value):
    def one(axis_at, blocks):
        heights = jax.random.uniform(jax.random.fold_in(jax.random.fold_in(stream_key, 6), axis_at), (blocks,), jnp.float32, low / len(cuts), top_value / len(cuts))
        return jnp.repeat(jnp.exp(heights), extent[axis_at] // blocks).reshape((-1,) + (1,) * (len(extent) - axis_at - 1))

    gain = one(*cuts[0])
    for cut in cuts[1:]:
        gain = gain * one(*cut)
    return gain


def centred(rng, shape, spread, most, shards=(), held_as=jnp.bfloat16):
    entries = jax.random.normal(rng, shape, jnp.float32) * spread
    if len(shards) > 0:
        entries = level_of(rng, shape, shards, -0.22, 0.18) * entries
    return jnp.clip(entries, min=-most, max=most).astype(held_as)


def setup_inputs(seed: int = 0) -> dict:
    seeds = jax.random.split(jax.random.key(seed), 6)
    return {
        "gains": centred(seeds[0], (S, CH, 8 * DIR), 1.0, 6.0, ((0, 32),), jnp.float32),
        "coherency": centred(seeds[1], (S, S, CH, TI, 8 * DIR), 1.0, 6.0, ((0, 4), (1, 8))),
        "cotangent": centred(seeds[2], (S, S, CH, TI, 8), 0.016, 0.099609375, ((0, 4), (1, 8))),
        "flags": plant((jax.random.randint(seeds[3], (S, S, TI), 0, 4) < 3).astype(jnp.int32), jax.random.fold_in(seeds[3], 1), 0, 1),
        "station_slot": draw_station_slot(jax.random.fold_in(seeds[5], 71), 0),
    }


def complex_product(first, second):
    return (first[0] * second[0] - first[1] * second[1], first[0] * second[1] + first[1] * second[0])


def complex_sum(first, second):
    return (first[0] + second[0], first[1] + second[1])


def conjugate(element):
    return (element[0], -element[1])


def jones_product(first, second):
    return [complex_sum(complex_product(first[2 * row_index], second[column]), complex_product(first[2 * row_index + 1], second[2 + column])) for row_index in (0, 1) for column in (0, 1)]


def hermitian(matrix):
    return [conjugate(matrix[0]), conjugate(matrix[2]), conjugate(matrix[1]), conjugate(matrix[3])]


def as_complex(parts):
    return [(parts[0], parts[1]), (parts[2], parts[3]), (parts[4], parts[5]), (parts[6], parts[7])]


def as_parts(matrix):
    return [number for element in matrix for number in element]


def block_gradients(coherency, cotangent, flags, row_gains, col_gains):
    shape = coherency.shape
    directions = shape[4] // 8
    coherence = coherency.reshape(shape[:4] + (8, directions))
    weight = flags.astype(jnp.float32)[:, :, None, :, None]
    residual = as_complex([cotangent[..., component].astype(jnp.float32)[..., None] * weight for component in range(8)])
    model_parts = as_complex([coherence[..., component, :].astype(jnp.float32) for component in range(8)])
    row_split = row_gains.reshape(row_gains.shape[0], row_gains.shape[1], 8, directions)
    col_split = col_gains.reshape(col_gains.shape[0], col_gains.shape[1], 8, directions)
    row_jones = as_complex([row_split[:, None, :, None, component, :] for component in range(8)])
    col_jones = as_complex([col_split[None, :, :, None, component, :] for component in range(8)])
    outgoing = jones_product(jones_product(residual, col_jones), hermitian(model_parts))
    row_side = jnp.stack([jnp.sum(part, axis=(1, 3)) for part in as_parts(outgoing)], axis=2)
    incoming = jones_product(jones_product(hermitian(residual), row_jones), model_parts)
    col_side = jnp.stack([jnp.sum(part, axis=(0, 3)) for part in as_parts(incoming)], axis=2)
    return row_side.reshape(row_gains.shape), col_side.reshape(col_gains.shape)


def reference(gains, coherency, cotangent, flags, station_slot):
    slot_gains = jnp.take(gains, station_slot, axis=0)
    block_rows = 16
    stations = gains.shape[0]

    def accumulate(totals, block_index):
        start = (block_index * block_rows).astype(jnp.int32)
        coher_rows = lax.dynamic_slice_in_dim(coherency, start, block_rows, 0)
        cotan_rows = lax.dynamic_slice_in_dim(cotangent, start, block_rows, 0)
        flag_rows = lax.dynamic_slice_in_dim(flags, start, block_rows, 0)
        gain_rows = lax.dynamic_slice_in_dim(slot_gains, start, block_rows, 0)
        row_side, col_side = block_gradients(coher_rows, cotan_rows, flag_rows, gain_rows, slot_gains)
        return totals + col_side, row_side

    indices = jnp.arange(stations // block_rows, dtype=jnp.int32)
    col_total, row_blocks = lax.scan(accumulate, jnp.zeros(gains.shape, gains.dtype), indices)
    slot_grad = row_blocks.reshape(gains.shape) + col_total
    return jnp.zeros(gains.shape, gains.dtype).at[station_slot].set(slot_grad)
```

```python
import functools

import jax
import jax.numpy as jnp
from jax import lax
from jax.experimental import pallas as pl
from jax.experimental.pallas import tpu as pltpu
from jax.sharding import PartitionSpec as P


def swap_pairs(values, width, even):
    return jnp.where(even, pltpu.roll(values, 3 * width, 1), pltpu.roll(values, width, 1))


def two_parts(values):
    high = values.astype(jnp.bfloat16)
    return high, (values - high.astype(jnp.float32)).astype(jnp.bfloat16)


def row_weights(gains, width, even, sign):
    lanes = 4 * width
    rows = []
    for b in range(2):
        half = gains[:, b * lanes : (b + 1) * lanes]
        rows += [half, -sign * swap_pairs(half, width, even)]
    tables = []
    for part in two_parts(jnp.concatenate(rows, axis=0)):
        zero = jnp.zeros_like(part)
        tables += [
            jnp.concatenate([part, zero], axis=1),
            jnp.concatenate([zero, part], axis=1),
        ]
    return jnp.concatenate(tables, axis=0)


def col_weights(gains, width, even, sign, group):
    lanes = 4 * width
    blocks = []
    for b in range(2):
        half = gains[:, b * lanes : (b + 1) * lanes]
        other = pltpu.roll(half, 2 * width, 1)
        rows = [[], []]
        for e in range(2):
            twice = jnp.where(group // 2 == e, half, other)
            rows[0].append(sign * twice)
            rows[1].append(swap_pairs(twice, width, even))
        blocks.append(
            jnp.concatenate([jnp.concatenate(row, axis=1) for row in rows], axis=0)
        )
    tables = []
    for part in range(2):
        for b in range(2):
            value = two_parts(blocks[b])[part]
            zero = jnp.zeros_like(value)
            tables += [
                jnp.concatenate([value, zero], axis=1),
                jnp.concatenate([zero, value], axis=1),
            ]
    return jnp.concatenate(tables, axis=0)


def gradient_kernel(
    width, block, tile, parts, m_ref, g_ref, jr_ref, jc_ref, r_ref, c_ref,
    m_buf, m_sem, gt_ref, wr_ref, wc_ref, sxa_ref, sxb_ref, sya_ref, syb_ref,
    xa_ref, xb_ref, ya_ref, yb_ref, acc_ref, racc_ref,
):
    first, channels = jr_ref.shape[:2]
    second = jc_ref.shape[0]
    lanes = 4 * width
    depth = gt_ref.shape[2]
    slots = m_buf.shape[0]
    ring = wc_ref.shape[0]
    tiles = second // tile
    blocks = first // block
    total = blocks * tiles
    rows_each = block // parts
    cols_each = tile // parts
    each = block // (tiles * parts)
    early = 4

    lane_f = lax.broadcasted_iota(jnp.int32, (channels, depth), 1) % channels
    sub_f = lax.broadcasted_iota(jnp.int32, (channels, depth), 0)
    diagonal = (lane_f == sub_f).astype(jnp.float32)
    group = lax.broadcasted_iota(jnp.int32, (channels, lanes), 1) // width
    even = group % 2 == 0
    sign = jnp.where(even, 1.0, -1.0)
    both = lax.broadcasted_iota(jnp.int32, (2 * channels, lanes), 1) // width
    even_both = both % 2 == 0

    def fetch(at):
        row = at // tiles * block
        col = at % tiles * tile
        return pltpu.make_async_copy(
            m_ref.at[pl.ds(row, block), pl.ds(col, tile)],
            m_buf.at[at % slots],
            m_sem.at[at % slots],
        )

    def table(at):
        return col_weights(jr_ref[at], width, even, sign, group)

    def places_of(at):
        at = jnp.minimum(at, total - 1)
        return at // tiles * block, at % tiles * tile

    def spread(at, j, sx_ref, sy_ref):
        row, col = places_of(at)
        for v in range(0, cols_each, 2):
            kk = j * cols_each + v
            for u in range(0, block, 2):
                wide = [
                    [
                        gt_ref[col + kk + z, pl.ds(row + u + w, 1)] * diagonal
                        for w in range(2)
                    ]
                    for z in range(2)
                ]
                for z in range(2):
                    pair = jnp.concatenate(wide[z], axis=0).astype(jnp.bfloat16)
                    sx_ref[kk + z, u * channels : (u + 2) * channels] = pair
                    pair = jnp.concatenate([wide[0][z], wide[1][z]], axis=0)
                    start = pl.multiple_of(kk * channels, 2 * channels)
                    sy_ref[u + z, pl.ds(start, 2 * channels)] = pair.astype(jnp.bfloat16)

    def products(at, j, sx_ref, sy_ref, x_ref, y_ref):
        row, col = places_of(at)
        for n in range(cols_each):
            kk = j * cols_each + n
            x_ref[kk] = jnp.dot(
                sx_ref[kk], wr_ref[col + kk], preferred_element_type=jnp.float32
            )
        for n in range(rows_each):
            ii = j * rows_each + n
            y_ref[ii] = jnp.dot(
                sy_ref[ii], wc_ref[(row + ii) % ring], preferred_element_type=jnp.float32
            )

    def combine(at, j, x_ref, y_ref):
        pair = 2
        slot = at % slots
        col_at = at % tiles * tile
        for half in range(rows_each // pair):
            base = j * rows_each + half * pair
            totals = [racc_ref[base + p, n] for p in range(pair) for n in range(8)]
            for q in range(tile):
                k = col_at + q
                col = [acc_ref[k, n] for n in range(4)]
                for p in range(pair):
                    m = m_buf[slot, base + p, q]
                    turned = jnp.where(
                        even_both,
                        pltpu.roll(m, 3 * width, 1),
                        pltpu.roll(m, width, 1),
                    )
                    wide = m.astype(jnp.float32)
                    halves = [wide[:channels], wide[channels:]]
                    wide = turned.astype(jnp.float32)
                    swapped = [wide[:channels], wide[channels:]]
                    start = pl.multiple_of((base + p) * channels, channels)
                    for a in range(2):
                        x = x_ref[q, pl.ds(start, channels), a * lanes : (a + 1) * lanes]
                        for c in range(2):
                            n = p * 8 + 4 * a + 2 * c
                            totals[n] = totals[n] + x * halves[c]
                            totals[n + 1] = totals[n + 1] + x * swapped[c]
                    for a in range(2):
                        for e in range(2):
                            n = 2 * a + e
                            y = y_ref[
                                base + p,
                                q * channels : (q + 1) * channels,
                                n * lanes : (n + 1) * lanes,
                            ]
                            col[2 * a] = col[2 * a] + y * halves[e]
                            col[2 * a + 1] = col[2 * a + 1] + y * swapped[e]
                for n in range(4):
                    acc_ref[k, n] = col[n]
            for p in range(pair):
                for n in range(8):
                    racc_ref[base + p, n] = totals[8 * p + n]

    for at in range(min(slots - 1, total)):
        fetch(at).start()
    acc_ref[...] = jnp.zeros_like(acc_ref)

    def turn(k, carry):
        rows = [g_ref[k, pl.ds(p, channels, stride=8)] for p in range(8)]
        gt_ref[k] = jnp.concatenate(rows * 2, axis=0).T
        return carry

    lax.fori_loop(0, second, turn, 0, unroll=4)

    def prepare(k, carry):
        wr_ref[k] = row_weights(jc_ref[k], width, even, sign)
        return carry

    lax.fori_loop(0, second, prepare, 0, unroll=8)

    def prepare_col(i, carry):
        wc_ref[i] = table(i)
        return carry

    lax.fori_loop(0, block + early, prepare_col, 0, unroll=4)

    def begin_spread(j, carry):
        spread(0, j, sxa_ref, sya_ref)
        spread(1, j, sxb_ref, syb_ref)
        return carry

    lax.fori_loop(0, parts, begin_spread, 0)

    def begin(j, carry):
        products(0, j, sxa_ref, sya_ref, xa_ref, ya_ref)
        return carry

    lax.fori_loop(0, parts, begin, 0)

    def phase(at, here, there):
        sx_here, sy_here, x_here, y_here = here
        sx_there, sy_there, x_there, y_there = there
        fetch(at).wait()

        @pl.when(at + slots - 1 < total)
        def _():
            fetch(at + slots - 1).start()

        def body(j, carry):
            products(at + 1, j, sx_there, sy_there, x_there, y_there)
            combine(at, j, x_here, y_here)
            spread(at + 2, j, sx_here, sy_here)
            step = at // tiles + 1
            for n in range(each):
                ahead = step * block + early + (at % tiles * parts + j) * each + n
                wc_ref[ahead % ring] = table(jnp.minimum(ahead, first - 1))
            return carry

        lax.fori_loop(0, parts, body, 0)

    a_side = (sxa_ref, sya_ref, xa_ref, ya_ref)
    b_side = (sxb_ref, syb_ref, xb_ref, yb_ref)

    def row_block(step, carry):
        racc_ref[...] = jnp.zeros_like(racc_ref)

        def two_tiles(t, carry):
            at = step * tiles + 2 * t
            phase(at, a_side, b_side)
            phase(at + 1, b_side, a_side)
            return carry

        lax.fori_loop(0, tiles // 2, two_tiles, 0)

        def settle(i, carry):
            for a in range(2):
                values = [racc_ref[i, 4 * a + n] for n in range(4)]
                values = [v if n % 2 == 0 else -sign * v for n, v in enumerate(values)]
                sums = []
                for n in (0, 2):
                    kept = jnp.where(even, values[n], values[n + 1])
                    moved = jnp.where(even, values[n + 1], values[n])
                    sums.append(kept + pltpu.roll(moved, width, 1))
                kept = jnp.where(group < 2, sums[0], sums[1])
                moved = jnp.where(group < 2, sums[1], sums[0])
                r_ref[step * block + i, :, a * lanes : (a + 1) * lanes] = (
                    kept + pltpu.roll(moved, 2 * width, 1)
                )
            return carry

        lax.fori_loop(0, block, settle, 0, unroll=8)
        return carry

    lax.fori_loop(0, blocks, row_block, 0)

    def finish(k, carry):
        for a in range(2):
            real = acc_ref[k, 2 * a]
            imag = acc_ref[k, 2 * a + 1] * sign
            kept = jnp.where(even, real, imag)
            moved = jnp.where(even, imag, real)
            c_ref[k, :, a * lanes : (a + 1) * lanes] = kept + swap_pairs(moved, width, even)
        return carry

    lax.fori_loop(0, second, finish, 0, unroll=8)


def residuals(cotangent, flags):
    first, second, channels = cotangent.shape[:3]
    kept = flags.astype(jnp.float32)[..., None]
    weighted = cotangent[:, :, :, 0].astype(jnp.float32) * kept
    return weighted.transpose(1, 2, 3, 0).reshape(second, 8 * channels, first)


def block_gradients(coherency, residual, row_gains, col_gains):
    first, second, channels, _, wide = coherency.shape
    width = wide // 8
    lanes = wide // 2
    block = 16
    tile = 16
    parts = 4
    slots = 4
    depth = 16 * channels
    f32, bf16 = jnp.float32, jnp.bfloat16
    model = coherency.reshape(first, second, channels, 2, lanes).transpose(0, 1, 3, 2, 4)
    model = model.reshape(first, second, 2 * channels, lanes)
    spread_x = pltpu.VMEM((tile, block * channels, depth), bf16)
    spread_y = pltpu.VMEM((block, tile * channels, depth), bf16)
    x_shape = pltpu.VMEM((tile, block * channels, wide), f32)
    y_shape = pltpu.VMEM((block, tile * channels, 2 * wide), f32)
    vmem = pl.BlockSpec(memory_space=pltpu.VMEM)
    return pl.pallas_call(
        functools.partial(gradient_kernel, width, block, tile, parts),
        in_specs=[pl.BlockSpec(memory_space=pl.ANY), vmem, vmem, vmem],
        out_specs=[vmem, vmem],
        out_shape=[
            jax.ShapeDtypeStruct((first, channels, wide), f32),
            jax.ShapeDtypeStruct((second, channels, wide), f32),
        ],
        scratch_shapes=[
            pltpu.VMEM((slots, block, tile, 2 * channels, lanes), bf16),
            pltpu.SemaphoreType.DMA((slots,)),
            pltpu.VMEM((second, first, depth), f32),
            pltpu.VMEM((second, depth, wide), bf16),
            pltpu.VMEM((2 * block, depth, 2 * wide), bf16),
            spread_x, spread_x, spread_y, spread_y, x_shape, x_shape, y_shape, y_shape,
            pltpu.VMEM((second, 4, channels, lanes), f32),
            pltpu.VMEM((block, 8, channels, lanes), f32),
        ],
        compiler_params=pltpu.CompilerParams(vmem_limit_bytes=58 * 1024 * 1024),
    )(model, residual, row_gains, col_gains)


MESH = pl.DeviceIdType.MESH


def device(place, col_total):
    return (place // col_total, place % col_total)


def remote(source, target, send_sem, recv_sem, where):
    return pltpu.make_async_remote_copy(
        src_ref=source,
        dst_ref=target,
        send_sem=send_sem,
        recv_sem=recv_sem,
        device_id=where,
        device_id_type=MESH,
    )


def each(start, stop, action):
    def body(index, carry):
        action(index)
        return carry

    lax.fori_loop(start, stop, body, 0)


def greet(me, total, col_total):
    barrier = pltpu.get_barrier_semaphore()

    def hello(offset):
        pl.semaphore_signal(
            barrier,
            inc=1,
            device_id=device(lax.rem(me + offset, total), col_total),
            device_id_type=MESH,
        )

    each(1, total, hello)
    pl.semaphore_wait(barrier, total - 1)


def exchange(send_ref, recv_ref, send_sems, recv_sems, me, total, col_total):
    def copy(offset):
        place = lax.rem(me + offset, total)
        return remote(
            send_ref.at[place],
            recv_ref.at[me],
            send_sems.at[offset],
            recv_sems.at[offset],
            device(place, col_total),
        )

    each(1, total, lambda offset: copy(offset).start())
    recv_ref[me] = send_ref[me]
    each(1, total, lambda offset: copy(offset).wait())


def spread_kernel(
    row_total, col_total, holders_ref, send_ref, row_ref, col_ref,
    recv_ref, x_send, x_recv, c_send, c_recv, a_send, a_recv, b_send, b_recv,
):
    share = holders_ref.shape[1]
    r = lax.axis_index("row")
    c = lax.axis_index("col")
    total = row_total * col_total
    me = r * col_total + c
    greet(me, total, col_total)
    exchange(send_ref, recv_ref, x_send, x_recv, me, total, col_total)

    def choose(j):
        row_ref[c * share + j] = recv_ref[holders_ref[0, j], 0]
        col_ref[r * share + j] = recv_ref[holders_ref[1, j], 1]

    each(0, share, choose)
    half = col_total // 2
    partner = c + 1 - 2 * (c % 2)

    def col_copy(offset):
        block = col_ref.at[pl.ds(r * share, share)]
        where = (lax.rem(r + offset, row_total), c)
        return remote(block, block, c_send.at[offset], c_recv.at[offset], where)

    def far_copy(offset):
        block = row_ref.at[pl.ds(c * share, share)]
        where = (r, lax.rem(c + 2 * offset, col_total))
        return remote(block, block, a_send.at[offset], a_recv.at[offset], where)

    def near_copy(offset):
        origin = lax.rem(c + col_total - 2 * offset, col_total)
        block = row_ref.at[pl.ds(origin * share, share)]
        return remote(block, block, b_send.at[offset], b_recv.at[offset], (r, partner))

    each(1, half, lambda offset: far_copy(offset).start())
    each(1, row_total, lambda offset: col_copy(offset).start())
    near_copy(0).start()

    def forward(offset):
        far_copy(offset).wait_recv()
        near_copy(offset).start()

    each(1, half, forward)
    each(1, half, lambda offset: far_copy(offset).wait_send())
    each(0, half, lambda offset: near_copy(offset).wait())
    each(1, row_total, lambda offset: col_copy(offset).wait())


def collect_kernel(
    row_total, col_total, back_ref, own_ref, row_ref, col_ref, out_ref,
    pair_ref, part_ref, far_ref, colin_ref, sums_ref, send_ref, recv_ref,
    x_send, x_recv, c_send, c_recv, a_send, a_recv, b_send, b_recv,
):
    share = own_ref.shape[1]
    r = lax.axis_index("row")
    c = lax.axis_index("col")
    total = row_total * col_total
    me = r * col_total + c
    half = col_total // 2
    core = c % 2
    chip = c // 2
    greet(me, total, col_total)

    def near_copy(offset):
        q = lax.rem(chip + offset, half)
        block = row_ref.at[pl.ds((2 * q + 1 - core) * share, share)]
        return remote(
            block, pair_ref.at[q], a_send.at[offset], a_recv.at[offset], (r, 2 * chip + 1 - core)
        )

    def far_copy(offset):
        q = lax.rem(chip + offset, half)
        return remote(
            part_ref.at[q], far_ref.at[offset], b_send.at[offset], b_recv.at[offset],
            (r, 2 * q + core),
        )

    def col_copy(offset):
        there = lax.rem(r + offset, row_total)
        block = col_ref.at[pl.ds(there * share, share)]
        return remote(
            block, colin_ref.at[offset], c_send.at[offset], c_recv.at[offset], (there, c)
        )

    def join(offset):
        near_copy(offset).wait_recv()
        q = lax.rem(chip + offset, half)
        part_ref[q] = row_ref[pl.ds((2 * q + core) * share, share)] + pair_ref[q]

    def join_and_send(offset):
        join(offset)
        far_copy(offset).start()

    each(1, half + 1, lambda offset: near_copy(lax.rem(offset, half)).start())
    each(1, row_total, lambda offset: col_copy(offset).start())
    each(1, half, join_and_send)
    join(0)
    sums_ref[0] = part_ref[chip]
    sums_ref[1] = col_ref[pl.ds(r * share, share)]

    def add_col(offset):
        col_copy(offset).wait()
        sums_ref[1] += colin_ref[offset]

    def add_row(offset):
        far_copy(offset).wait()
        sums_ref[0] += far_ref[offset]

    each(1, row_total, add_col)
    each(1, half, add_row)
    each(0, half, lambda offset: near_copy(offset).wait_send())

    def address(place):
        send_ref[place, 0] = sums_ref[0, back_ref[0, place]]
        send_ref[place, 1] = sums_ref[1, back_ref[1, place]]

    each(0, total, address)
    exchange(send_ref, recv_ref, x_send, x_recv, me, total, col_total)

    def settle(j):
        out_ref[j] = recv_ref[own_ref[0, j], 0] + recv_ref[own_ref[1, j], 1]

    each(0, share, settle)


def semaphores(total, row_total, col_total):
    counts = (total, row_total, col_total // 2, col_total // 2)
    return [pltpu.SemaphoreType.DMA((count,)) for count in counts for _ in range(2)]


def places(identifiers, count):
    here = identifiers[:, None] == jnp.arange(count, dtype=jnp.int32)[None, :]
    index = jnp.arange(identifiers.shape[0], dtype=jnp.int32)[:, None]
    return jnp.sum(jnp.where(here, index, 0), axis=0, dtype=jnp.int32)


def call_options(identifier):
    return pltpu.CompilerParams(collective_id=identifier, has_side_effects=True)


def shards(gains, coherency, cotangent, flags, station_slot):
    stations = station_slot.shape[0]
    share = gains.shape[0]
    tail = gains.shape[1:]
    row_total = lax.axis_size("row")
    col_total = lax.axis_size("col")
    groups = row_total * col_total
    row_place = lax.axis_index("row")
    col_place = lax.axis_index("col")
    device_place = row_place * col_total + col_place
    counting = jnp.arange(share, dtype=jnp.int32)
    mine = device_place * share + counting
    found = station_slot[None, :] == mine[:, None]
    slot_index = jnp.arange(stations, dtype=jnp.int32)[None, :]
    own_blocks = jnp.sum(jnp.where(found, slot_index, 0), axis=1, dtype=jnp.int32) // share
    col_target = own_blocks % row_total * col_total + own_blocks // row_total
    col_block = col_place * row_total + row_place
    row_holder = lax.dynamic_slice_in_dim(station_slot, device_place * share, share) // share
    col_holder = lax.dynamic_slice_in_dim(station_slot, col_block * share, share) // share
    holders = jnp.stack([row_holder, col_holder])
    targets = jnp.stack([own_blocks, col_target])
    picks = jnp.stack([places(own_blocks, groups), places(col_target, groups)], axis=1)
    sent = jnp.take(gains, picks.reshape(-1), axis=0).reshape((groups, 2) + tail)
    vmem = pl.BlockSpec(memory_space=pltpu.VMEM)
    smem = pl.BlockSpec(memory_space=pltpu.SMEM)
    f32 = jnp.float32
    table = pltpu.VMEM((groups, 2) + tail, f32)
    row_gains, col_gains = pl.pallas_call(
        functools.partial(spread_kernel, row_total, col_total),
        in_specs=[smem, vmem],
        out_specs=[vmem, vmem],
        out_shape=[
            jax.ShapeDtypeStruct((col_total * share,) + tail, f32),
            jax.ShapeDtypeStruct((row_total * share,) + tail, f32),
        ],
        scratch_shapes=[table] + semaphores(groups, row_total, col_total),
        compiler_params=call_options(1),
    )(holders, sent)
    row_side, col_side = block_gradients(
        coherency, residuals(cotangent, flags), row_gains, col_gains
    )
    backs = jnp.stack([places(row_holder, groups), places(col_holder, groups)])
    half = col_total // 2
    return pl.pallas_call(
        functools.partial(collect_kernel, row_total, col_total),
        in_specs=[smem, smem, vmem, vmem],
        out_specs=vmem,
        out_shape=jax.ShapeDtypeStruct(gains.shape, f32),
        scratch_shapes=[
            pltpu.VMEM((half, share) + tail, f32),
            pltpu.VMEM((half, share) + tail, f32),
            pltpu.VMEM((half, share) + tail, f32),
            pltpu.VMEM((row_total, share) + tail, f32),
            pltpu.VMEM((2, share) + tail, f32),
            table,
            table,
        ]
        + semaphores(groups, row_total, col_total),
        compiler_params=call_options(2),
    )(backs, targets, row_side, col_side)


def solution(mesh):
    placed = (
        P(("row", "col"), None, None),
        P("row", "col", None, None, None),
        P("row", "col", None, None, None),
        P("row", "col", None),
        P(),
    )
    return jax.shard_map(
        shards, mesh=mesh, in_specs=placed, out_specs=P(("row", "col"), None, None), check_vma=False
    )
```

```python
import functools

import jax
import jax.numpy as jnp
from jax import lax
from jax.experimental import pallas as pl
from jax.experimental.pallas import tpu as pltpu
from jax.sharding import PartitionSpec as P


def swap_pairs(values, width, even):
    return jnp.where(even, pltpu.roll(values, 3 * width, 1), pltpu.roll(values, width, 1))


def two_parts(values):
    high = values.astype(jnp.bfloat16)
    return high, (values - high.astype(jnp.float32)).astype(jnp.bfloat16)


def row_weights(gains, width, even, sign):
    lanes = 4 * width
    rows = []
    for b in range(2):
        half = gains[:, b * lanes : (b + 1) * lanes]
        rows += [half, -sign * swap_pairs(half, width, even)]
    tables = []
    for part in two_parts(jnp.concatenate(rows, axis=0)):
        zero = jnp.zeros_like(part)
        tables += [
            jnp.concatenate([part, zero], axis=1),
            jnp.concatenate([zero, part], axis=1),
        ]
    return jnp.concatenate(tables, axis=0)


def col_weights(gains, width, even, sign, group):
    lanes = 4 * width
    blocks = []
    for b in range(2):
        half = gains[:, b * lanes : (b + 1) * lanes]
        other = pltpu.roll(half, 2 * width, 1)
        rows = [[], []]
        for e in range(2):
            twice = jnp.where(group // 2 == e, half, other)
            rows[0].append(sign * twice)
            rows[1].append(swap_pairs(twice, width, even))
        blocks.append(
            jnp.concatenate([jnp.concatenate(row, axis=1) for row in rows], axis=0)
        )
    tables = []
    for part in range(2):
        for b in range(2):
            value = two_parts(blocks[b])[part]
            zero = jnp.zeros_like(value)
            tables += [
                jnp.concatenate([value, zero], axis=1),
                jnp.concatenate([zero, value], axis=1),
            ]
    return jnp.concatenate(tables, axis=0)


def gradient_kernel(
    width, block, tile, parts, m_ref, g_ref, jr_ref, jc_ref, r_ref, c_ref,
    m_buf, m_sem, gt_ref, wr_ref, wc_ref, sxa_ref, sxb_ref, sya_ref, syb_ref,
    xa_ref, xb_ref, ya_ref, yb_ref, acc_ref, racc_ref,
):
    first, channels = jr_ref.shape[:2]
    second = jc_ref.shape[0]
    lanes = 4 * width
    depth = gt_ref.shape[2]
    slots = m_buf.shape[0]
    ring = wc_ref.shape[0]
    tiles = second // tile
    blocks = first // block
    total = blocks * tiles
    rows_each = block // parts
    cols_each = tile // parts
    each = block // (tiles * parts)
    early = 4

    lane_f = lax.broadcasted_iota(jnp.int32, (channels, depth), 1) % channels
    sub_f = lax.broadcasted_iota(jnp.int32, (channels, depth), 0)
    diagonal = (lane_f == sub_f).astype(jnp.float32)
    group = lax.broadcasted_iota(jnp.int32, (channels, lanes), 1) // width
    even = group % 2 == 0
    sign = jnp.where(even, 1.0, -1.0)
    both = lax.broadcasted_iota(jnp.int32, (2 * channels, lanes), 1) // width
    even_both = both % 2 == 0

    def fetch(at):
        row = at // tiles * block
        col = at % tiles * tile
        return pltpu.make_async_copy(
            m_ref.at[pl.ds(row, block), pl.ds(col, tile)],
            m_buf.at[at % slots],
            m_sem.at[at % slots],
        )

    def table(at):
        return col_weights(jr_ref[at], width, even, sign, group)

    def places_of(at):
        at = jnp.minimum(at, total - 1)
        return at // tiles * block, at % tiles * tile

    def spread(at, j, sx_ref, sy_ref):
        row, col = places_of(at)
        for v in range(0, cols_each, 2):
            kk = j * cols_each + v
            for u in range(0, block, 2):
                wide = [
                    [
                        gt_ref[col + kk + z, pl.ds(row + u + w, 1)] * diagonal
                        for w in range(2)
                    ]
                    for z in range(2)
                ]
                for z in range(2):
                    pair = jnp.concatenate(wide[z], axis=0).astype(jnp.bfloat16)
                    sx_ref[kk + z, u * channels : (u + 2) * channels] = pair
                    pair = jnp.concatenate([wide[0][z], wide[1][z]], axis=0)
                    start = pl.multiple_of(kk * channels, 2 * channels)
                    sy_ref[u + z, pl.ds(start, 2 * channels)] = pair.astype(jnp.bfloat16)

    def products(at, j, sx_ref, sy_ref, x_ref, y_ref):
        row, col = places_of(at)
        for n in range(cols_each):
            kk = j * cols_each + n
            x_ref[kk] = jnp.dot(
                sx_ref[kk], wr_ref[col + kk], preferred_element_type=jnp.float32
            )
        for n in range(rows_each):
            ii = j * rows_each + n
            y_ref[ii] = jnp.dot(
                sy_ref[ii], wc_ref[(row + ii) % ring], preferred_element_type=jnp.float32
            )

    def combine(at, j, x_ref, y_ref):
        pair = 2
        slot = at % slots
        col_at = at % tiles * tile
        for half in range(rows_each // pair):
            base = j * rows_each + half * pair
            totals = [racc_ref[base + p, n] for p in range(pair) for n in range(8)]
            for q in range(tile):
                k = col_at + q
                col = [acc_ref[k, n] for n in range(4)]
                for p in range(pair):
                    m = m_buf[slot, base + p, q]
                    turned = jnp.where(
                        even_both,
                        pltpu.roll(m, 3 * width, 1),
                        pltpu.roll(m, width, 1),
                    )
                    wide = m.astype(jnp.float32)
                    halves = [wide[:channels], wide[channels:]]
                    wide = turned.astype(jnp.float32)
                    swapped = [wide[:channels], wide[channels:]]
                    start = pl.multiple_of((base + p) * channels, channels)
                    for a in range(2):
                        x = x_ref[q, pl.ds(start, channels), a * lanes : (a + 1) * lanes]
                        for c in range(2):
                            n = p * 8 + 4 * a + 2 * c
                            totals[n] = totals[n] + x * halves[c]
                            totals[n + 1] = totals[n + 1] + x * swapped[c]
                    for a in range(2):
                        for e in range(2):
                            n = 2 * a + e
                            y = y_ref[
                                base + p,
                                q * channels : (q + 1) * channels,
                                n * lanes : (n + 1) * lanes,
                            ]
                            col[2 * a] = col[2 * a] + y * halves[e]
                            col[2 * a + 1] = col[2 * a + 1] + y * swapped[e]
                for n in range(4):
                    acc_ref[k, n] = col[n]
            for p in range(pair):
                for n in range(8):
                    racc_ref[base + p, n] = totals[8 * p + n]

    for at in range(min(slots - 1, total)):
        fetch(at).start()
    acc_ref[...] = jnp.zeros_like(acc_ref)

    def turn(k, carry):
        rows = [g_ref[k, pl.ds(p, channels, stride=8)] for p in range(8)]
        gt_ref[k] = jnp.concatenate(rows * 2, axis=0).T
        return carry

    lax.fori_loop(0, second, turn, 0, unroll=8)

    def prepare(k, carry):
        wr_ref[k] = row_weights(jc_ref[k], width, even, sign)
        return carry

    lax.fori_loop(0, second, prepare, 0, unroll=8)

    def prepare_col(i, carry):
        wc_ref[i] = table(i)
        return carry

    lax.fori_loop(0, block + early, prepare_col, 0, unroll=4)

    def begin_spread(j, carry):
        spread(0, j, sxa_ref, sya_ref)
        spread(1, j, sxb_ref, syb_ref)
        return carry

    lax.fori_loop(0, parts, begin_spread, 0)

    def begin(j, carry):
        products(0, j, sxa_ref, sya_ref, xa_ref, ya_ref)
        return carry

    lax.fori_loop(0, parts, begin, 0)

    def phase(at, here, there):
        sx_here, sy_here, x_here, y_here = here
        sx_there, sy_there, x_there, y_there = there
        fetch(at).wait()

        @pl.when(at + slots - 1 < total)
        def _():
            fetch(at + slots - 1).start()

        def body(j, carry):
            products(at + 1, j, sx_there, sy_there, x_there, y_there)
            combine(at, j, x_here, y_here)
            spread(at + 2, j, sx_here, sy_here)
            step = at // tiles + 1
            for n in range(each):
                ahead = step * block + early + (at % tiles * parts + j) * each + n
                wc_ref[ahead % ring] = table(jnp.minimum(ahead, first - 1))
            return carry

        lax.fori_loop(0, parts, body, 0)

    a_side = (sxa_ref, sya_ref, xa_ref, ya_ref)
    b_side = (sxb_ref, syb_ref, xb_ref, yb_ref)

    def row_block(step, carry):
        racc_ref[...] = jnp.zeros_like(racc_ref)

        def two_tiles(t, carry):
            at = step * tiles + 2 * t
            phase(at, a_side, b_side)
            phase(at + 1, b_side, a_side)
            return carry

        lax.fori_loop(0, tiles // 2, two_tiles, 0)

        def settle(i, carry):
            for a in range(2):
                values = [racc_ref[i, 4 * a + n] for n in range(4)]
                values = [v if n % 2 == 0 else -sign * v for n, v in enumerate(values)]
                sums = []
                for n in (0, 2):
                    kept = jnp.where(even, values[n], values[n + 1])
                    moved = jnp.where(even, values[n + 1], values[n])
                    sums.append(kept + pltpu.roll(moved, width, 1))
                kept = jnp.where(group < 2, sums[0], sums[1])
                moved = jnp.where(group < 2, sums[1], sums[0])
                r_ref[step * block + i, :, a * lanes : (a + 1) * lanes] = (
                    kept + pltpu.roll(moved, 2 * width, 1)
                )
            return carry

        lax.fori_loop(0, block, settle, 0, unroll=8)
        return carry

    lax.fori_loop(0, blocks, row_block, 0)

    def finish(k, carry):
        for a in range(2):
            real = acc_ref[k, 2 * a]
            imag = acc_ref[k, 2 * a + 1] * sign
            kept = jnp.where(even, real, imag)
            moved = jnp.where(even, imag, real)
            c_ref[k, :, a * lanes : (a + 1) * lanes] = kept + swap_pairs(moved, width, even)
        return carry

    lax.fori_loop(0, second, finish, 0, unroll=8)


def residuals(cotangent, flags):
    first, second, channels = cotangent.shape[:3]
    kept = flags.astype(jnp.float32)[..., None]
    weighted = cotangent[:, :, :, 0].astype(jnp.float32) * kept
    return weighted.transpose(1, 2, 3, 0).reshape(second, 8 * channels, first)


def block_gradients(coherency, residual, row_gains, col_gains):
    first, second, channels, _, wide = coherency.shape
    width = wide // 8
    lanes = wide // 2
    block = 8
    tile = min(32, second // 2)
    parts = 1
    slots = 4
    depth = 16 * channels
    f32, bf16 = jnp.float32, jnp.bfloat16
    model = coherency.reshape(first, second, channels, 2, lanes).transpose(0, 1, 3, 2, 4)
    model = model.reshape(first, second, 2 * channels, lanes)
    spread_x = pltpu.VMEM((tile, block * channels, depth), bf16)
    spread_y = pltpu.VMEM((block, tile * channels, depth), bf16)
    x_shape = pltpu.VMEM((tile, block * channels, wide), f32)
    y_shape = pltpu.VMEM((block, tile * channels, 2 * wide), f32)
    vmem = pl.BlockSpec(memory_space=pltpu.VMEM)
    return pl.pallas_call(
        functools.partial(gradient_kernel, width, block, tile, parts),
        in_specs=[pl.BlockSpec(memory_space=pl.ANY), vmem, vmem, vmem],
        out_specs=[vmem, vmem],
        out_shape=[
            jax.ShapeDtypeStruct((first, channels, wide), f32),
            jax.ShapeDtypeStruct((second, channels, wide), f32),
        ],
        scratch_shapes=[
            pltpu.VMEM((slots, block, tile, 2 * channels, lanes), bf16),
            pltpu.SemaphoreType.DMA((slots,)),
            pltpu.VMEM((second, first, depth), f32),
            pltpu.VMEM((second, depth, wide), bf16),
            pltpu.VMEM((2 * block, depth, 2 * wide), bf16),
            spread_x, spread_x, spread_y, spread_y, x_shape, x_shape, y_shape, y_shape,
            pltpu.VMEM((second, 4, channels, lanes), f32),
            pltpu.VMEM((block, 8, channels, lanes), f32),
        ],
        compiler_params=pltpu.CompilerParams(vmem_limit_bytes=58 * 1024 * 1024),
    )(model, residual, row_gains, col_gains)


MESH = pl.DeviceIdType.MESH


def device(place, col_total):
    return (place // col_total, place % col_total)


def remote(source, target, send_sem, recv_sem, where):
    return pltpu.make_async_remote_copy(
        src_ref=source,
        dst_ref=target,
        send_sem=send_sem,
        recv_sem=recv_sem,
        device_id=where,
        device_id_type=MESH,
    )


def each(start, stop, action):
    def body(index, carry):
        action(index)
        return carry

    lax.fori_loop(start, stop, body, 0)


def greet(me, total, col_total):
    barrier = pltpu.get_barrier_semaphore()

    def hello(offset):
        pl.semaphore_signal(
            barrier,
            inc=1,
            device_id=device(lax.rem(me + offset, total), col_total),
            device_id_type=MESH,
        )

    each(1, total, hello)
    pl.semaphore_wait(barrier, total - 1)


def exchange(send_ref, recv_ref, send_sems, recv_sems, me, total, col_total):
    def copy(offset):
        place = lax.rem(me + offset, total)
        return remote(
            send_ref.at[place],
            recv_ref.at[me],
            send_sems.at[offset],
            recv_sems.at[offset],
            device(place, col_total),
        )

    each(1, total, lambda offset: copy(offset).start())
    recv_ref[me] = send_ref[me]
    each(1, total, lambda offset: copy(offset).wait())


def spread_kernel(
    row_total, col_total, table_ref, sent_ref, row_ref, col_ref,
    send_ref, load_sem, recv_ref, x_send, x_recv, c_send, c_recv, a_send, a_recv, b_send, b_recv,
):
    share = row_ref.shape[0] // col_total
    r = lax.axis_index("row")
    c = lax.axis_index("col")
    total = row_total * col_total
    me = r * col_total + c
    load = pltpu.make_async_copy(sent_ref, send_ref, load_sem.at[0])
    load.start()
    greet(me, total, col_total)
    load.wait()
    exchange(send_ref, recv_ref, x_send, x_recv, me, total, col_total)

    def choose(j):
        row_ref[c * share + j] = recv_ref[table_ref[j], 0]
        col_ref[r * share + j] = recv_ref[table_ref[share + j], 1]

    each(0, share, choose)
    half = col_total // 2
    partner = c + 1 - 2 * (c % 2)

    def col_copy(offset):
        block = col_ref.at[pl.ds(r * share, share)]
        where = (lax.rem(r + offset, row_total), c)
        return remote(block, block, c_send.at[offset], c_recv.at[offset], where)

    def far_copy(offset):
        block = row_ref.at[pl.ds(c * share, share)]
        where = (r, lax.rem(c + 2 * offset, col_total))
        return remote(block, block, a_send.at[offset], a_recv.at[offset], where)

    def near_copy(offset):
        origin = lax.rem(c + col_total - 2 * offset, col_total)
        block = row_ref.at[pl.ds(origin * share, share)]
        return remote(block, block, b_send.at[offset], b_recv.at[offset], (r, partner))

    each(1, half, lambda offset: far_copy(offset).start())
    each(1, row_total, lambda offset: col_copy(offset).start())
    near_copy(0).start()

    def forward(offset):
        far_copy(offset).wait_recv()
        near_copy(offset).start()

    each(1, half, forward)
    each(1, half, lambda offset: far_copy(offset).wait_send())
    each(0, half, lambda offset: near_copy(offset).wait())
    each(1, row_total, lambda offset: col_copy(offset).wait())


def collect_kernel(
    row_total, col_total, table_ref, rows_ref, cols_ref, out_ref,
    row_ref, col_ref, load_sem, pair_ref, part_ref, far_ref, colin_ref, sums_ref, send_ref, recv_ref,
    x_send, x_recv, c_send, c_recv, a_send, a_recv, b_send, b_recv,
):
    share = out_ref.shape[0]
    r = lax.axis_index("row")
    c = lax.axis_index("col")
    total = row_total * col_total
    me = r * col_total + c
    half = col_total // 2
    core = c % 2
    chip = c // 2
    load_rows = pltpu.make_async_copy(rows_ref, row_ref, load_sem.at[0])
    load_cols = pltpu.make_async_copy(cols_ref, col_ref, load_sem.at[1])
    load_rows.start()
    load_cols.start()
    greet(me, total, col_total)
    load_rows.wait()
    load_cols.wait()

    def near_copy(offset):
        q = lax.rem(chip + offset, half)
        block = row_ref.at[pl.ds((2 * q + 1 - core) * share, share)]
        return remote(
            block, pair_ref.at[q], a_send.at[offset], a_recv.at[offset], (r, 2 * chip + 1 - core)
        )

    def far_copy(offset):
        q = lax.rem(chip + offset, half)
        return remote(
            part_ref.at[q], far_ref.at[offset], b_send.at[offset], b_recv.at[offset],
            (r, 2 * q + core),
        )

    def col_copy(offset):
        there = lax.rem(r + offset, row_total)
        block = col_ref.at[pl.ds(there * share, share)]
        return remote(
            block, colin_ref.at[offset], c_send.at[offset], c_recv.at[offset], (there, c)
        )

    def join(offset):
        near_copy(offset).wait_recv()
        q = lax.rem(chip + offset, half)
        part_ref[q] = row_ref[pl.ds((2 * q + core) * share, share)] + pair_ref[q]

    def join_and_send(offset):
        join(offset)
        far_copy(offset).start()

    each(1, half + 1, lambda offset: near_copy(lax.rem(offset, half)).start())
    each(1, row_total, lambda offset: col_copy(offset).start())
    each(1, half, join_and_send)
    join(0)
    sums_ref[0] = part_ref[chip]
    sums_ref[1] = col_ref[pl.ds(r * share, share)]

    def add_col(offset):
        col_copy(offset).wait()
        sums_ref[1] += colin_ref[offset]

    def add_row(offset):
        far_copy(offset).wait()
        sums_ref[0] += far_ref[offset]

    each(1, row_total, add_col)
    each(1, half, add_row)
    each(0, half, lambda offset: near_copy(offset).wait_send())

    def address(place):
        send_ref[place, 0] = sums_ref[0, table_ref[4 * share + place]]
        send_ref[place, 1] = sums_ref[1, table_ref[4 * share + total + place]]

    each(0, total, address)
    exchange(send_ref, recv_ref, x_send, x_recv, me, total, col_total)

    def settle(j):
        out_ref[j] = recv_ref[table_ref[2 * share + j], 0] + recv_ref[table_ref[3 * share + j], 1]

    each(0, share, settle)


def semaphores(total, row_total, col_total):
    counts = (total, row_total, col_total // 2, col_total // 2)
    return [pltpu.SemaphoreType.DMA((count,)) for count in counts for _ in range(2)]


def places(identifiers, count):
    here = identifiers[:, None] == jnp.arange(count, dtype=jnp.int32)[None, :]
    index = jnp.arange(identifiers.shape[0], dtype=jnp.int32)[:, None]
    return jnp.sum(jnp.where(here, index, 0), axis=0, dtype=jnp.int32)


def call_options(identifier):
    return pltpu.CompilerParams(collective_id=identifier, has_side_effects=True)


def shards(gains, coherency, cotangent, flags, station_slot):
    stations = station_slot.shape[0]
    share = gains.shape[0]
    tail = gains.shape[1:]
    row_total = lax.axis_size("row")
    col_total = lax.axis_size("col")
    groups = row_total * col_total
    row_place = lax.axis_index("row")
    col_place = lax.axis_index("col")
    device_place = row_place * col_total + col_place
    counting = jnp.arange(share, dtype=jnp.int32)
    mine = device_place * share + counting
    found = station_slot[None, :] == mine[:, None]
    slot_index = jnp.arange(stations, dtype=jnp.int32)[None, :]
    own_blocks = jnp.sum(jnp.where(found, slot_index, 0), axis=1, dtype=jnp.int32) // share
    col_target = own_blocks % row_total * col_total + own_blocks // row_total
    col_block = col_place * row_total + row_place
    row_holder = lax.dynamic_slice_in_dim(station_slot, device_place * share, share) // share
    col_holder = lax.dynamic_slice_in_dim(station_slot, col_block * share, share) // share
    numbers = jnp.concatenate(
        [
            row_holder,
            col_holder,
            own_blocks,
            col_target,
            places(row_holder, groups),
            places(col_holder, groups),
        ]
    )
    picks = jnp.stack([places(own_blocks, groups), places(col_target, groups)], axis=1)
    sent = jnp.take(gains, picks.reshape(-1), axis=0, mode="clip").reshape((groups, 2) + tail)
    vmem = pl.BlockSpec(memory_space=pltpu.VMEM)
    smem = pl.BlockSpec(memory_space=pltpu.SMEM)
    f32 = jnp.float32
    table = pltpu.VMEM((groups, 2) + tail, f32)
    row_gains, col_gains = pl.pallas_call(
        functools.partial(spread_kernel, row_total, col_total),
        in_specs=[smem, pl.BlockSpec(memory_space=pl.ANY)],
        out_specs=[vmem, vmem],
        out_shape=[
            jax.ShapeDtypeStruct((col_total * share,) + tail, f32),
            jax.ShapeDtypeStruct((row_total * share,) + tail, f32),
        ],
        scratch_shapes=[table, pltpu.SemaphoreType.DMA((1,)), table] + semaphores(groups, row_total, col_total),
        compiler_params=call_options(1),
    )(numbers, sent)
    row_side, col_side = block_gradients(
        coherency, residuals(cotangent, flags), row_gains, col_gains
    )
    half = col_total // 2
    return pl.pallas_call(
        functools.partial(collect_kernel, row_total, col_total),
        in_specs=[smem] + [pl.BlockSpec(memory_space=pl.ANY)] * 2,
        out_specs=vmem,
        out_shape=jax.ShapeDtypeStruct(gains.shape, f32),
        scratch_shapes=[
            pltpu.VMEM(row_side.shape, f32),
            pltpu.VMEM(col_side.shape, f32),
            pltpu.SemaphoreType.DMA((2,)),
            pltpu.VMEM((half, share) + tail, f32),
            pltpu.VMEM((half, share) + tail, f32),
            pltpu.VMEM((half, share) + tail, f32),
            pltpu.VMEM((row_total, share) + tail, f32),
            pltpu.VMEM((2, share) + tail, f32),
            table,
            table,
        ]
        + semaphores(groups, row_total, col_total),
        compiler_params=call_options(2),
    )(numbers, row_side, col_side)


def solution(mesh):
    placed = (
        P(("row", "col"), None, None),
        P("row", "col", None, None, None),
        P("row", "col", None, None, None),
        P("row", "col", None),
        P(),
    )
    return jax.shard_map(
        shards, mesh=mesh, in_specs=placed, out_specs=P(("row", "col"), None, None), check_vma=False
    )
```

```python
import functools

import jax
import jax.numpy as jnp
from jax import lax
from jax.experimental import pallas as pl
from jax.experimental.pallas import tpu as pltpu
from jax.sharding import PartitionSpec as P


def swap_pairs(values, width, even):
    return jnp.where(even, pltpu.roll(values, 3 * width, 1), pltpu.roll(values, width, 1))


def two_parts(values):
    high = values.astype(jnp.bfloat16)
    return high, (values - high.astype(jnp.float32)).astype(jnp.bfloat16)


def row_weights(gains, width, even, sign):
    lanes = 4 * width
    rows = []
    for b in range(2):
        half = gains[:, b * lanes : (b + 1) * lanes]
        rows += [half, -sign * swap_pairs(half, width, even)]
    tables = []
    for part in two_parts(jnp.concatenate(rows, axis=0)):
        zero = jnp.zeros_like(part)
        tables += [
            jnp.concatenate([part, zero], axis=1),
            jnp.concatenate([zero, part], axis=1),
        ]
    return jnp.concatenate(tables, axis=0)


def col_weights(gains, width, even, sign, group):
    lanes = 4 * width
    blocks = []
    for b in range(2):
        half = gains[:, b * lanes : (b + 1) * lanes]
        other = pltpu.roll(half, 2 * width, 1)
        rows = [[], []]
        for e in range(2):
            twice = jnp.where(group // 2 == e, half, other)
            rows[0].append(sign * twice)
            rows[1].append(swap_pairs(twice, width, even))
        blocks.append(
            jnp.concatenate([jnp.concatenate(row, axis=1) for row in rows], axis=0)
        )
    tables = []
    for part in range(2):
        for b in range(2):
            value = two_parts(blocks[b])[part]
            zero = jnp.zeros_like(value)
            tables += [
                jnp.concatenate([value, zero], axis=1),
                jnp.concatenate([zero, value], axis=1),
            ]
    return jnp.concatenate(tables, axis=0)


def gradient_kernel(
    width, block, tile, parts, m_ref, g_ref, jr_ref, jc_ref, r_ref, c_ref,
    m_buf, m_sem, gt_ref, wr_ref, wc_ref, sxa_ref, sxb_ref, sya_ref, syb_ref,
    xa_ref, xb_ref, ya_ref, yb_ref, acc_ref, racc_ref,
):
    first, channels = jr_ref.shape[:2]
    second = jc_ref.shape[0]
    lanes = 4 * width
    depth = gt_ref.shape[2]
    slots = m_buf.shape[0]
    ring = wc_ref.shape[0]
    tiles = second // tile
    blocks = first // block
    total = blocks * tiles
    rows_each = block // parts
    cols_each = tile // parts
    each = block // (tiles * parts)
    early = 4

    lane_f = lax.broadcasted_iota(jnp.int32, (channels, depth), 1) % channels
    sub_f = lax.broadcasted_iota(jnp.int32, (channels, depth), 0)
    diagonal = (lane_f == sub_f).astype(jnp.float32)
    group = lax.broadcasted_iota(jnp.int32, (channels, lanes), 1) // width
    even = group % 2 == 0
    sign = jnp.where(even, 1.0, -1.0)
    both = lax.broadcasted_iota(jnp.int32, (2 * channels, lanes), 1) // width
    even_both = both % 2 == 0

    def fetch(at):
        row = at // tiles * block
        col = at % tiles * tile
        return pltpu.make_async_copy(
            m_ref.at[pl.ds(row, block), pl.ds(col, tile)],
            m_buf.at[at % slots],
            m_sem.at[at % slots],
        )

    def table(at):
        return col_weights(jr_ref[at], width, even, sign, group)

    def places_of(at):
        at = jnp.minimum(at, total - 1)
        return at // tiles * block, at % tiles * tile

    def spread(at, j, sx_ref, sy_ref):
        row, col = places_of(at)
        for v in range(0, cols_each, 2):
            kk = j * cols_each + v
            for u in range(0, block, 2):
                wide = [
                    [
                        gt_ref[col + kk + z, pl.ds(row + u + w, 1)] * diagonal
                        for w in range(2)
                    ]
                    for z in range(2)
                ]
                for z in range(2):
                    pair = jnp.concatenate(wide[z], axis=0).astype(jnp.bfloat16)
                    sx_ref[kk + z, u * channels : (u + 2) * channels] = pair
                    pair = jnp.concatenate([wide[0][z], wide[1][z]], axis=0)
                    start = pl.multiple_of(kk * channels, 2 * channels)
                    sy_ref[u + z, pl.ds(start, 2 * channels)] = pair.astype(jnp.bfloat16)

    def products(at, j, sx_ref, sy_ref, x_ref, y_ref):
        row, col = places_of(at)
        for n in range(cols_each):
            kk = j * cols_each + n
            x_ref[kk] = jnp.dot(
                sx_ref[kk], wr_ref[col + kk], preferred_element_type=jnp.float32
            )
        for n in range(rows_each):
            ii = j * rows_each + n
            y_ref[ii] = jnp.dot(
                sy_ref[ii], wc_ref[(row + ii) % ring], preferred_element_type=jnp.float32
            )

    def combine(at, j, x_ref, y_ref):
        pair = 2
        slot = at % slots
        col_at = at % tiles * tile
        for half in range(rows_each // pair):
            base = j * rows_each + half * pair
            totals = [racc_ref[base + p, n] for p in range(pair) for n in range(8)]
            for q in range(tile):
                k = col_at + q
                col = [acc_ref[k, n] for n in range(4)]
                for p in range(pair):
                    m = m_buf[slot, base + p, q]
                    turned = jnp.where(
                        even_both,
                        pltpu.roll(m, 3 * width, 1),
                        pltpu.roll(m, width, 1),
                    )
                    wide = m.astype(jnp.float32)
                    halves = [wide[:channels], wide[channels:]]
                    wide = turned.astype(jnp.float32)
                    swapped = [wide[:channels], wide[channels:]]
                    start = pl.multiple_of((base + p) * channels, channels)
                    for a in range(2):
                        x = x_ref[q, pl.ds(start, channels), a * lanes : (a + 1) * lanes]
                        for c in range(2):
                            n = p * 8 + 4 * a + 2 * c
                            totals[n] = totals[n] + x * halves[c]
                            totals[n + 1] = totals[n + 1] + x * swapped[c]
                    for a in range(2):
                        for e in range(2):
                            n = 2 * a + e
                            y = y_ref[
                                base + p,
                                q * channels : (q + 1) * channels,
                                n * lanes : (n + 1) * lanes,
                            ]
                            col[2 * a] = col[2 * a] + y * halves[e]
                            col[2 * a + 1] = col[2 * a + 1] + y * swapped[e]
                for n in range(4):
                    acc_ref[k, n] = col[n]
            for p in range(pair):
                for n in range(8):
                    racc_ref[base + p, n] = totals[8 * p + n]

    for at in range(min(slots - 1, total)):
        fetch(at).start()
    acc_ref[...] = jnp.zeros_like(acc_ref)

    def turn(k, carry):
        rows = [g_ref[k, pl.ds(p, channels, stride=8)] for p in range(8)]
        gt_ref[k] = jnp.concatenate(rows * 2, axis=0).T
        return carry

    lax.fori_loop(0, second, turn, 0, unroll=8)

    def prepare(k, carry):
        wr_ref[k] = row_weights(jc_ref[k], width, even, sign)
        return carry

    lax.fori_loop(0, second, prepare, 0, unroll=8)

    def prepare_col(i, carry):
        wc_ref[i] = table(i)
        return carry

    lax.fori_loop(0, block + early, prepare_col, 0, unroll=4)

    def begin_spread(j, carry):
        spread(0, j, sxa_ref, sya_ref)
        spread(1, j, sxb_ref, syb_ref)
        return carry

    lax.fori_loop(0, parts, begin_spread, 0)

    def begin(j, carry):
        products(0, j, sxa_ref, sya_ref, xa_ref, ya_ref)
        return carry

    lax.fori_loop(0, parts, begin, 0)

    def phase(at, here, there):
        sx_here, sy_here, x_here, y_here = here
        sx_there, sy_there, x_there, y_there = there
        fetch(at).wait()

        @pl.when(at + slots - 1 < total)
        def _():
            fetch(at + slots - 1).start()

        def body(j, carry):
            products(at + 1, j, sx_there, sy_there, x_there, y_there)
            combine(at, j, x_here, y_here)
            spread(at + 2, j, sx_here, sy_here)
            step = at // tiles + 1
            for n in range(each):
                ahead = step * block + early + (at % tiles * parts + j) * each + n
                wc_ref[ahead % ring] = table(jnp.minimum(ahead, first - 1))
            return carry

        lax.fori_loop(0, parts, body, 0)

    a_side = (sxa_ref, sya_ref, xa_ref, ya_ref)
    b_side = (sxb_ref, syb_ref, xb_ref, yb_ref)

    def row_block(step, carry):
        racc_ref[...] = jnp.zeros_like(racc_ref)

        def two_tiles(t, carry):
            at = step * tiles + 2 * t
            phase(at, a_side, b_side)
            phase(at + 1, b_side, a_side)
            return carry

        lax.fori_loop(0, tiles // 2, two_tiles, 0)

        def settle(i, carry):
            for a in range(2):
                values = [racc_ref[i, 4 * a + n] for n in range(4)]
                values = [v if n % 2 == 0 else -sign * v for n, v in enumerate(values)]
                sums = []
                for n in (0, 2):
                    kept = jnp.where(even, values[n], values[n + 1])
                    moved = jnp.where(even, values[n + 1], values[n])
                    sums.append(kept + pltpu.roll(moved, width, 1))
                kept = jnp.where(group < 2, sums[0], sums[1])
                moved = jnp.where(group < 2, sums[1], sums[0])
                r_ref[step * block + i, :, a * lanes : (a + 1) * lanes] = (
                    kept + pltpu.roll(moved, 2 * width, 1)
                )
            return carry

        lax.fori_loop(0, block, settle, 0, unroll=8)
        return carry

    lax.fori_loop(0, blocks, row_block, 0)

    def finish(k, carry):
        for a in range(2):
            real = acc_ref[k, 2 * a]
            imag = acc_ref[k, 2 * a + 1] * sign
            kept = jnp.where(even, real, imag)
            moved = jnp.where(even, imag, real)
            c_ref[k, :, a * lanes : (a + 1) * lanes] = kept + swap_pairs(moved, width, even)
        return carry

    lax.fori_loop(0, second, finish, 0, unroll=8)


def residuals(cotangent, flags):
    first, second, channels = cotangent.shape[:3]
    kept = flags.astype(jnp.float32)[..., None]
    weighted = cotangent[:, :, :, 0].astype(jnp.float32) * kept
    return weighted.transpose(1, 2, 3, 0).reshape(second, 8 * channels, first)


def block_gradients(coherency, residual, row_gains, col_gains):
    first, second, channels, _, wide = coherency.shape
    width = wide // 8
    lanes = wide // 2
    block = 8
    tile = min(32, second // 2)
    parts = 1
    slots = 4
    depth = 16 * channels
    f32, bf16 = jnp.float32, jnp.bfloat16
    model = coherency.reshape(first, second, channels, 2, lanes).transpose(0, 1, 3, 2, 4)
    model = model.reshape(first, second, 2 * channels, lanes)
    spread_x = pltpu.VMEM((tile, block * channels, depth), bf16)
    spread_y = pltpu.VMEM((block, tile * channels, depth), bf16)
    x_shape = pltpu.VMEM((tile, block * channels, wide), f32)
    y_shape = pltpu.VMEM((block, tile * channels, 2 * wide), f32)
    vmem = pl.BlockSpec(memory_space=pltpu.VMEM)
    return pl.pallas_call(
        functools.partial(gradient_kernel, width, block, tile, parts),
        in_specs=[pl.BlockSpec(memory_space=pl.ANY), vmem, vmem, vmem],
        out_specs=[vmem, vmem],
        out_shape=[
            jax.ShapeDtypeStruct((first, channels, wide), f32),
            jax.ShapeDtypeStruct((second, channels, wide), f32),
        ],
        scratch_shapes=[
            pltpu.VMEM((slots, block, tile, 2 * channels, lanes), bf16),
            pltpu.SemaphoreType.DMA((slots,)),
            pltpu.VMEM((second, first, depth), f32),
            pltpu.VMEM((second, depth, wide), bf16),
            pltpu.VMEM((2 * block, depth, 2 * wide), bf16),
            spread_x, spread_x, spread_y, spread_y, x_shape, x_shape, y_shape, y_shape,
            pltpu.VMEM((second, 4, channels, lanes), f32),
            pltpu.VMEM((block, 8, channels, lanes), f32),
        ],
        compiler_params=pltpu.CompilerParams(vmem_limit_bytes=58 * 1024 * 1024),
    )(model, residual, row_gains, col_gains)


MESH = pl.DeviceIdType.MESH


def device(place, col_total):
    return (place // col_total, place % col_total)


def remote(source, target, send_sem, recv_sem, where):
    return pltpu.make_async_remote_copy(
        src_ref=source,
        dst_ref=target,
        send_sem=send_sem,
        recv_sem=recv_sem,
        device_id=where,
        device_id_type=MESH,
    )


def each(start, stop, action):
    def body(index, carry):
        action(index)
        return carry

    lax.fori_loop(start, stop, body, 0)


def greet(me, total, col_total):
    barrier = pltpu.get_barrier_semaphore()

    def hello(offset):
        pl.semaphore_signal(
            barrier,
            inc=1,
            device_id=device(lax.rem(me + offset, total), col_total),
            device_id_type=MESH,
        )

    each(1, total, hello)
    pl.semaphore_wait(barrier, total - 1)


def exchange(send_ref, recv_ref, send_sems, recv_sems, me, total, col_total):
    def copy(offset):
        place = lax.rem(me + offset, total)
        return remote(
            send_ref.at[place],
            recv_ref.at[me],
            send_sems.at[offset],
            recv_sems.at[offset],
            device(place, col_total),
        )

    each(1, total, lambda offset: copy(offset).start())
    recv_ref[me] = send_ref[me]
    return lambda: each(1, total, lambda offset: copy(offset).wait())


def spread_kernel(
    row_total, col_total, table_ref, sent_ref, row_ref, col_ref,
    send_ref, load_sem, recv_row_ref, recv_col_ref,
    x_send, x_recv, y_send, y_recv, c_send, c_recv, a_send, a_recv, b_send, b_recv,
):
    share = row_ref.shape[0] // col_total
    r = lax.axis_index("row")
    c = lax.axis_index("col")
    total = row_total * col_total
    me = r * col_total + c
    load = pltpu.make_async_copy(sent_ref, send_ref, load_sem.at[0])
    load.start()
    greet(me, total, col_total)
    load.wait()
    row_done = exchange(
        send_ref.at[0], recv_row_ref, x_send, x_recv, me, total, col_total
    )
    col_done = exchange(
        send_ref.at[1], recv_col_ref, y_send, y_recv, me, total, col_total
    )
    row_done()

    def choose_row(j):
        row_ref[c * share + j] = recv_row_ref[table_ref[j]]

    def choose_col(j):
        col_ref[r * share + j] = recv_col_ref[table_ref[share + j]]

    each(0, share, choose_row)
    half = col_total // 2
    partner = c + 1 - 2 * (c % 2)

    def col_copy(offset):
        block = col_ref.at[pl.ds(r * share, share)]
        where = (lax.rem(r + offset, row_total), c)
        return remote(block, block, c_send.at[offset], c_recv.at[offset], where)

    def far_copy(offset):
        block = row_ref.at[pl.ds(c * share, share)]
        where = (r, lax.rem(c + 2 * offset, col_total))
        return remote(block, block, a_send.at[offset], a_recv.at[offset], where)

    def near_copy(offset):
        origin = lax.rem(c + col_total - 2 * offset, col_total)
        block = row_ref.at[pl.ds(origin * share, share)]
        return remote(block, block, b_send.at[offset], b_recv.at[offset], (r, partner))

    each(1, half, lambda offset: far_copy(offset).start())
    near_copy(0).start()
    col_done()
    each(0, share, choose_col)
    each(1, row_total, lambda offset: col_copy(offset).start())

    def forward(offset):
        far_copy(offset).wait_recv()
        near_copy(offset).start()

    each(1, half, forward)
    each(1, half, lambda offset: far_copy(offset).wait_send())
    each(0, half, lambda offset: near_copy(offset).wait())
    each(1, row_total, lambda offset: col_copy(offset).wait())


def collect_kernel(
    row_total, col_total, table_ref, rows_ref, cols_ref, out_ref,
    row_ref, col_ref, load_sem, pair_ref, part_ref, far_ref, colin_ref, row_sum_ref, col_sum_ref,
    send_row_ref, send_col_ref, recv_row_ref, recv_col_ref,
    x_send, x_recv, y_send, y_recv, c_send, c_recv, a_send, a_recv, b_send, b_recv,
):
    share = out_ref.shape[0]
    r = lax.axis_index("row")
    c = lax.axis_index("col")
    total = row_total * col_total
    me = r * col_total + c
    half = col_total // 2
    core = c % 2
    chip = c // 2
    load_rows = pltpu.make_async_copy(rows_ref, row_ref, load_sem.at[0])
    load_cols = pltpu.make_async_copy(cols_ref, col_ref, load_sem.at[1])
    load_rows.start()
    load_cols.start()
    greet(me, total, col_total)
    load_rows.wait()
    load_cols.wait()

    def near_copy(offset):
        q = lax.rem(chip + offset, half)
        block = row_ref.at[pl.ds((2 * q + 1 - core) * share, share)]
        return remote(
            block, pair_ref.at[q], a_send.at[offset], a_recv.at[offset], (r, 2 * chip + 1 - core)
        )

    def far_copy(offset):
        q = lax.rem(chip + offset, half)
        return remote(
            part_ref.at[q], far_ref.at[offset], b_send.at[offset], b_recv.at[offset],
            (r, 2 * q + core),
        )

    def col_copy(offset):
        there = lax.rem(r + offset, row_total)
        block = col_ref.at[pl.ds(there * share, share)]
        return remote(
            block, colin_ref.at[offset], c_send.at[offset], c_recv.at[offset], (there, c)
        )

    def join(offset):
        near_copy(offset).wait_recv()
        q = lax.rem(chip + offset, half)
        part_ref[q] = row_ref[pl.ds((2 * q + core) * share, share)] + pair_ref[q]

    def join_and_send(offset):
        join(offset)
        far_copy(offset).start()

    each(1, half + 1, lambda offset: near_copy(lax.rem(offset, half)).start())
    each(1, row_total, lambda offset: col_copy(offset).start())
    each(1, half, join_and_send)
    join(0)
    col_sum_ref[...] = col_ref[pl.ds(r * share, share)]

    def add_col(offset):
        col_copy(offset).wait()
        col_sum_ref[...] += colin_ref[offset]

    def add_row(offset):
        far_copy(offset).wait()
        row_sum_ref[...] += far_ref[offset]

    def address_col(place):
        send_col_ref[place] = col_sum_ref[table_ref[4 * share + total + place]]

    def address_row(place):
        send_row_ref[place] = row_sum_ref[table_ref[4 * share + place]]

    each(1, row_total, add_col)
    each(0, total, address_col)
    col_done = exchange(send_col_ref, recv_col_ref, y_send, y_recv, me, total, col_total)
    row_sum_ref[...] = part_ref[chip]
    each(1, half, add_row)
    each(0, half, lambda offset: near_copy(offset).wait_send())
    each(0, total, address_row)
    row_done = exchange(send_row_ref, recv_row_ref, x_send, x_recv, me, total, col_total)
    col_done()
    row_done()

    def settle(j):
        out_ref[j] = (
            recv_row_ref[table_ref[2 * share + j]] + recv_col_ref[table_ref[3 * share + j]]
        )

    each(0, share, settle)


def semaphores(total, row_total, col_total):
    counts = (total, total, row_total, col_total // 2, col_total // 2)
    return [pltpu.SemaphoreType.DMA((count,)) for count in counts for _ in range(2)]


def places(identifiers, count):
    here = identifiers[:, None] == jnp.arange(count, dtype=jnp.int32)[None, :]
    index = jnp.arange(identifiers.shape[0], dtype=jnp.int32)[:, None]
    return jnp.sum(jnp.where(here, index, 0), axis=0, dtype=jnp.int32)


def call_options(identifier):
    return pltpu.CompilerParams(collective_id=identifier, has_side_effects=True)


def shards(gains, coherency, cotangent, flags, station_slot):
    stations = station_slot.shape[0]
    share = gains.shape[0]
    tail = gains.shape[1:]
    row_total = lax.axis_size("row")
    col_total = lax.axis_size("col")
    groups = row_total * col_total
    row_place = lax.axis_index("row")
    col_place = lax.axis_index("col")
    device_place = row_place * col_total + col_place
    counting = jnp.arange(share, dtype=jnp.int32)
    mine = device_place * share + counting
    found = station_slot[None, :] == mine[:, None]
    slot_index = jnp.arange(stations, dtype=jnp.int32)[None, :]
    own_blocks = jnp.sum(jnp.where(found, slot_index, 0), axis=1, dtype=jnp.int32) // share
    col_target = own_blocks % row_total * col_total + own_blocks // row_total
    col_block = col_place * row_total + row_place
    row_holder = lax.dynamic_slice_in_dim(station_slot, device_place * share, share) // share
    col_holder = lax.dynamic_slice_in_dim(station_slot, col_block * share, share) // share
    numbers = jnp.concatenate(
        [
            row_holder,
            col_holder,
            own_blocks,
            col_target,
            places(row_holder, groups),
            places(col_holder, groups),
        ]
    )
    picks = jnp.concatenate([places(own_blocks, groups), places(col_target, groups)])
    sent = jnp.take(gains, picks, axis=0, mode="clip").reshape((2, groups) + tail)
    vmem = pl.BlockSpec(memory_space=pltpu.VMEM)
    smem = pl.BlockSpec(memory_space=pltpu.SMEM)
    f32 = jnp.float32
    table = pltpu.VMEM((groups,) + tail, f32)
    row_gains, col_gains = pl.pallas_call(
        functools.partial(spread_kernel, row_total, col_total),
        in_specs=[smem, pl.BlockSpec(memory_space=pl.ANY)],
        out_specs=[vmem, vmem],
        out_shape=[
            jax.ShapeDtypeStruct((col_total * share,) + tail, f32),
            jax.ShapeDtypeStruct((row_total * share,) + tail, f32),
        ],
        scratch_shapes=[
            pltpu.VMEM((2, groups) + tail, f32),
            pltpu.SemaphoreType.DMA((1,)),
            table,
            table,
        ]
        + semaphores(groups, row_total, col_total),
        compiler_params=call_options(1),
    )(numbers, sent)
    row_side, col_side = block_gradients(
        coherency, residuals(cotangent, flags), row_gains, col_gains
    )
    half = col_total // 2
    return pl.pallas_call(
        functools.partial(collect_kernel, row_total, col_total),
        in_specs=[smem] + [pl.BlockSpec(memory_space=pl.ANY)] * 2,
        out_specs=vmem,
        out_shape=jax.ShapeDtypeStruct(gains.shape, f32),
        scratch_shapes=[
            pltpu.VMEM(row_side.shape, f32),
            pltpu.VMEM(col_side.shape, f32),
            pltpu.SemaphoreType.DMA((2,)),
            pltpu.VMEM((half, share) + tail, f32),
            pltpu.VMEM((half, share) + tail, f32),
            pltpu.VMEM((half, share) + tail, f32),
            pltpu.VMEM((row_total, share) + tail, f32),
            pltpu.VMEM((share,) + tail, f32),
            pltpu.VMEM((share,) + tail, f32),
            table,
            table,
            table,
            table,
        ]
        + semaphores(groups, row_total, col_total),
        compiler_params=call_options(2),
    )(numbers, row_side, col_side)


def solution(mesh):
    placed = (
        P(("row", "col"), None, None),
        P("row", "col", None, None, None),
        P("row", "col", None, None, None),
        P("row", "col", None),
        P(),
    )
    return jax.shard_map(
        shards, mesh=mesh, in_specs=placed, out_specs=P(("row", "col"), None, None), check_vma=False
    )
```
